32 devices in a mesh: fsdp: 8 (over z, y), model: 4 (over x, core).
Axes of the slice: x: 2, y: 2, z: 4, core: 2. Of those that a mesh axis runs over, the one named last changes fastest.
Arguments:
- x_in: bfloat16 [32, 64, 3584], P('fsdp', 'model')
- gain_attn: float32 [2, 3584], replicated
- gain_mlp: float32 [2, 3584], replicated
- rope_cos: float32 [64, 128], replicated
- rope_sin: float32 [64, 128], replicated
- w_q: bfloat16 [2, 3584, 4096], P(None, 'fsdp', 'model')
- w_k: bfloat16 [2, 3584, 2048], P(None, 'fsdp', 'model')
- w_v: bfloat16 [2, 3584, 2048], P(None, 'fsdp', 'model')
- w_o: bfloat16 [2, 4096, 3584], P(None, 'model', 'fsdp')
- w_gate: bfloat16 [2, 3584, 14336], P(None, 'fsdp', 'model')
- w_up: bfloat16 [2, 3584, 14336], P(None, 'fsdp', 'model')
- w_down: bfloat16 [2, 14336, 3584], P(None, 'model', 'fsdp')
Outputs:
- output: bfloat16 [32, 64, 3584], P('fsdp', 'model')
All inputs are finite; a program needn't handle non-finite values.
Results may differ from the reference program's by a relative error of at most 0.02.
Values are sent between devices in bfloat16 or wider.
A program may use at most 1 GiB of HBM per device.

```python
import math
import jax
import jax.numpy as jnp
from jax import lax

D_MODEL = 3584
FFN = 14336
HEADS = 16
KV_HEADS = 8
HEAD_DIM = 256
BATCH = 32
SEQ = 64
LAYERS = 2
EPS = 1e-5
ROPE_BASE = 500000.0


def rope_tables(rng_key):
    pos_steps = jax.random.randint(rng_key, (SEQ,), 1, 4)
    positions = (jnp.cumsum(pos_steps) - pos_steps[0]).astype(jnp.float32)
    inv_freq = ROPE_BASE ** (-jnp.arange(HEAD_DIM // 2, dtype=jnp.float32) * (2.0 / HEAD_DIM))
    angles = positions[:, None] * inv_freq[None, :]
    return jnp.cos(angles), jnp.sin(angles)


def setup_inputs(seed: int = 0) -> dict:
    key_list = jax.random.split(jax.random.key(seed), 12)
    q_scale = math.sqrt(max(1.0, math.log(SEQ / 16.0)))

    def normal(rng_key, arr_shape, std_scale):
        return (jax.random.normal(rng_key, arr_shape, jnp.float32) * std_scale).astype(jnp.bfloat16)

    rope_cos, rope_sin = rope_tables(key_list[3])
    return {
        'x_in': normal(key_list[0], (BATCH, SEQ, D_MODEL), 1.0),
        'gain_attn': jax.random.uniform(key_list[1], (LAYERS, D_MODEL), jnp.float32, 0.5, 1.5),
        'gain_mlp': jax.random.uniform(key_list[2], (LAYERS, D_MODEL), jnp.float32, 0.5, 1.5),
        'rope_cos': rope_cos,
        'rope_sin': rope_sin,
        'w_q': normal(key_list[4], (LAYERS, D_MODEL, HEADS * HEAD_DIM), q_scale * D_MODEL ** -0.5),
        'w_k': normal(key_list[5], (LAYERS, D_MODEL, KV_HEADS * HEAD_DIM), D_MODEL ** -0.5),
        'w_v': normal(key_list[6], (LAYERS, D_MODEL, KV_HEADS * HEAD_DIM), D_MODEL ** -0.5),
        'w_o': normal(key_list[7], (LAYERS, HEADS * HEAD_DIM, D_MODEL), 2.0 * (HEADS * HEAD_DIM) ** -0.5),
        'w_gate': normal(key_list[8], (LAYERS, D_MODEL, FFN), D_MODEL ** -0.5),
        'w_up': normal(key_list[9], (LAYERS, D_MODEL, FFN), D_MODEL ** -0.5),
        'w_down': normal(key_list[10], (LAYERS, FFN, D_MODEL), FFN ** -0.5),
    }


def rms_norm(seq_rows, gain_vec):
    rows_f = seq_rows.astype(jnp.float32)
    mean_sq = jnp.mean(rows_f * rows_f, axis=-1, keepdims=True)
    return (rows_f * lax.rsqrt(mean_sq + EPS) * gain_vec).astype(jnp.bfloat16)


def rotate(head_vals, cos_b, sin_b):
    half_dim = head_vals.shape[-1] // 2
    heads_f = head_vals.astype(jnp.float32)
    first_half = heads_f[..., :half_dim]
    second_half = heads_f[..., half_dim:]
    return jnp.concatenate([first_half * cos_b - second_half * sin_b, second_half * cos_b + first_half * sin_b], axis=-1).astype(jnp.bfloat16)


def decoder_layer(seq_rows, params, rope_cos, rope_sin):
    gain_attn, gain_mlp, w_q, w_k, w_v, w_o, w_gate, w_up, w_down = params
    group_size = HEADS // KV_HEADS
    normed = rms_norm(seq_rows, gain_attn)
    q_proj = jnp.dot(normed, w_q, preferred_element_type=jnp.float32).astype(jnp.bfloat16).reshape(SEQ, KV_HEADS, group_size, HEAD_DIM)
    k_proj = jnp.dot(normed, w_k, preferred_element_type=jnp.float32).astype(jnp.bfloat16).reshape(SEQ, KV_HEADS, HEAD_DIM)
    v_proj = jnp.dot(normed, w_v, preferred_element_type=jnp.float32).astype(jnp.bfloat16).reshape(SEQ, KV_HEADS, HEAD_DIM)
    q_rot = rotate(q_proj, rope_cos[:, None, None, :], rope_sin[:, None, None, :])
    k_rot = rotate(k_proj, rope_cos[:, None, :], rope_sin[:, None, :])
    scores = jnp.einsum('qkgd,skd->kgqs', q_rot.astype(jnp.float32), k_rot.astype(jnp.float32)) * HEAD_DIM ** -0.5
    positions = jnp.arange(SEQ)
    causal = positions[:, None] >= positions[None, :]
    scores = jnp.where(causal, scores, -jnp.inf)
    attn_probs = jax.nn.softmax(scores, axis=-1).astype(jnp.bfloat16)
    attn_out = jnp.einsum('kgqs,skd->qkgd', attn_probs.astype(jnp.float32), v_proj.astype(jnp.float32)).astype(jnp.bfloat16).reshape(SEQ, HEADS * HEAD_DIM)
    attn_sum = jnp.dot(attn_out, w_o, preferred_element_type=jnp.float32)
    mid_rows = (seq_rows.astype(jnp.float32) + attn_sum).astype(jnp.bfloat16)
    normed_mlp = rms_norm(mid_rows, gain_mlp)
    gate_acc = jnp.dot(normed_mlp, w_gate, preferred_element_type=jnp.float32)
    up_acc = jnp.dot(normed_mlp, w_up, preferred_element_type=jnp.float32)
    hidden = (jax.nn.silu(gate_acc) * up_acc).astype(jnp.bfloat16)
    mlp_sum = jnp.dot(hidden, w_down, preferred_element_type=jnp.float32)
    return (mid_rows.astype(jnp.float32) + mlp_sum).astype(jnp.bfloat16)


def reference(x_in, gain_attn, gain_mlp, rope_cos, rope_sin, w_q, w_k, w_v, w_o, w_gate, w_up, w_down):
    params = (gain_attn, gain_mlp, w_q, w_k, w_v, w_o, w_gate, w_up, w_down)

    def one_sequence(seq_rows):
        def layer_step(carry_rows, layer_params):
            return decoder_layer(carry_rows, layer_params, rope_cos, rope_sin), None
        final_rows, _ = lax.scan(layer_step, seq_rows, params)
        return final_rows

    return lax.map(one_sequence, x_in)
```

```python
import jax
import jax.numpy as jnp
from jax import lax
from jax.sharding import PartitionSpec as P

EPS = 1e-5


def rms_norm(rows, gain):
    rows_f = rows.astype(jnp.float32)
    mean_sq = jnp.mean(rows_f * rows_f, axis=-1, keepdims=True)
    return (rows_f * lax.rsqrt(mean_sq + EPS) * gain).astype(jnp.bfloat16)


def rotate(heads, cos, sin):
    half = heads.shape[-1] // 2
    heads_f = heads.astype(jnp.float32)
    a, b = heads_f[..., :half], heads_f[..., half:]
    return jnp.concatenate([a * cos - b * sin, b * cos + a * sin], axis=-1).astype(jnp.bfloat16)


def solution(mesh):
    n_f, n_m = mesh.shape['fsdp'], mesh.shape['model']
    act_spec = P('fsdp', 'model', None)
    col_spec = P(None, 'fsdp', 'model')
    row_spec = P(None, 'model', 'fsdp')

    def device_step(x_in, gain_attn, gain_mlp, rope_cos, rope_sin, w_q, w_k, w_v, w_o, w_gate, w_up, w_down):
        n_b, n_s, d = x_in.shape
        seq = n_s * n_m
        hd = 2 * rope_cos.shape[1]
        kv = w_k.shape[-1] // hd
        grp = w_q.shape[-1] // (hd * kv)
        rows = n_b * n_s
        d_f = d // n_f

        def shuffle_cols(w):
            return lax.all_to_all(w, 'fsdp', split_axis=1, concat_axis=0, tiled=True)

        def everyone(r):
            return lax.all_gather(r, ('model', 'fsdp'), axis=0, tiled=True)

        def matmul(a, b):
            return jnp.dot(a, b, preferred_element_type=jnp.float32)

        def return_rows(part, residual):
            total = lax.psum_scatter(part, 'model', scatter_dimension=0, tiled=True)
            mine = (residual + total).astype(jnp.bfloat16)
            return mine, lax.all_to_all(mine, 'fsdp', split_axis=0, concat_axis=1, tiled=True)

        my_rows = x_in.reshape(rows, d)
        residual = lax.all_to_all(my_rows, 'fsdp', split_axis=1, concat_axis=0, tiled=True)
        for l in range(w_q.shape[0]):
            w_qkv = shuffle_cols(jnp.concatenate([w_q[l], w_k[l], w_v[l]], axis=1))
            w_gu = shuffle_cols(jnp.concatenate([w_gate[l].reshape(d_f, n_f, -1), w_up[l].reshape(d_f, n_f, -1)], axis=2)).reshape(d, -1)
            h = rms_norm(everyone(my_rows), gain_attn[l])
            qkv = matmul(h, w_qkv).astype(jnp.bfloat16).reshape(n_m, n_f, rows, hd)
            qkv = lax.all_to_all(qkv, 'fsdp', split_axis=1, concat_axis=3, tiled=True)
            qkv = qkv.reshape(n_m, n_b, n_s, -1).transpose(1, 0, 2, 3).reshape(n_b, seq, -1)
            q = qkv[..., :kv * grp * hd].reshape(n_b, seq, kv, grp, hd)
            k = qkv[..., kv * grp * hd:kv * (grp + 1) * hd].reshape(n_b, seq, kv, hd)
            v = qkv[..., kv * (grp + 1) * hd:].reshape(n_b, seq, kv, hd)
            q = rotate(q, rope_cos[None, :, None, None, :], rope_sin[None, :, None, None, :])
            k = rotate(k, rope_cos[None, :, None, :], rope_sin[None, :, None, :])
            scores = jnp.einsum('bqkgd,bskd->bkgqs', q, k, preferred_element_type=jnp.float32) * hd ** -0.5
            pos = jnp.arange(seq)
            scores = jnp.where(pos[:, None] >= pos[None, :], scores, -jnp.inf)
            probs = jax.nn.softmax(scores, axis=-1).astype(jnp.bfloat16)
            o = jnp.einsum('bkgqs,bskd->bqkgd', probs, v, preferred_element_type=jnp.float32).astype(jnp.bfloat16)
            o = o.reshape(n_b, n_m, n_s, -1).transpose(1, 0, 2, 3).reshape(n_m, rows, -1)
            o = lax.all_gather(o, 'fsdp', axis=1, tiled=True).reshape(n_m * n_f * rows, -1)
            residual, my_rows = return_rows(matmul(o, w_o[l]), residual.astype(jnp.float32))
            u = rms_norm(everyone(my_rows), gain_mlp[l])
            gu = matmul(u, w_gu)
            z = (jax.nn.silu(gu[:, :gu.shape[1] // 2]) * gu[:, gu.shape[1] // 2:]).astype(jnp.bfloat16)
            z = lax.all_gather(z, 'fsdp', axis=1, tiled=True)
            residual, my_rows = return_rows(matmul(z, w_down[l]), residual.astype(jnp.float32))
        return my_rows.reshape(n_b, n_s, d)

    return jax.shard_map(device_step, mesh=mesh, in_specs=(act_spec, P(), P(), P(), P(), col_spec, col_spec, col_spec, row_spec, col_spec, col_spec, row_spec), out_specs=act_spec, check_vma=False)
```

```python
import functools

import jax
import jax.numpy as jnp
from jax import lax
from jax.experimental import pallas as pl
from jax.experimental.pallas import tpu as pltpu
from jax.sharding import PartitionSpec as P

EPS = 1e-5
MESH = pl.DeviceIdType.MESH
RIGHT, LEFT = 1, -1


def rms_norm(rows, gain, axis=-1):
    rows_f = rows.astype(jnp.float32)
    mean_sq = jnp.mean(rows_f * rows_f, axis=axis, keepdims=True)
    return (rows_f * lax.rsqrt(mean_sq + EPS) * gain).astype(jnp.bfloat16)


def rotate(heads, cos, sin):
    half = heads.shape[-1] // 2
    heads_f = heads.astype(jnp.float32)
    a, b = heads_f[..., :half], heads_f[..., half:]
    return jnp.concatenate([a * cos - b * sin, b * cos + a * sin], axis=-1).astype(jnp.bfloat16)


def ring_place(f):
    y, z = f % 2, f // 2
    return z * (1 - y) + (7 - z) * y


def ring_member(r):
    h = r // 4
    return 2 * (r * (1 - h) + (7 - r) * h) + h


class Copies:
    def __init__(self, send_sem, recv_sem):
        self.send_sem, self.recv_sem, self.made = send_sem, recv_sem, {}

    def start(self, name, src, dst, device):
        k = len(self.made)
        copy = pltpu.make_async_remote_copy(src_ref=src, dst_ref=dst, send_sem=self.send_sem.at[k], recv_sem=self.recv_sem.at[k], device_id=device, device_id_type=MESH)
        copy.start()
        self.made[name] = copy

    def arrived(self, name):
        self.made[name].wait_recv()

    def all_sent(self):
        for copy in self.made.values():
            copy.wait_send()


def greet(devices):
    barrier = pltpu.get_barrier_semaphore()
    for device in devices:
        pl.semaphore_signal(barrier, inc=1, device_id=device, device_id_type=MESH)
    pl.semaphore_wait(barrier, len(devices))


def group_kernel(place, n_pieces, x_ref, out_ref, send_sem, recv_sem, own_sem):
    f, m = lax.axis_index('fsdp'), lax.axis_index('model')
    r = ring_place(f)
    to = {d: (ring_member((r + d + 8) % 8), m) for d in (RIGHT, LEFT)}
    copies = Copies(send_sem, recv_sem)

    def at(origin, p):
        return place(out_ref, ring_member((origin + 8) % 8), p)

    def own(p):
        return place(x_ref, None, p)

    greet([to[RIGHT], to[LEFT]])
    for p in range(n_pieces):
        for d in (RIGHT, LEFT):
            copies.start((d, 1, p), own(p), at(r, p), to[d])
    mine = [pltpu.make_async_copy(own(p), at(r, p), own_sem.at[p]) for p in range(n_pieces)]
    for copy in mine:
        copy.start()
    last = {RIGHT: range(n_pieces // 2), LEFT: range(n_pieces // 2, n_pieces)}
    for step in (1, 2, 3):
        for p in range(n_pieces):
            for d in (RIGHT, LEFT):
                copies.arrived((d, step, p))
                if step < 3 or p in last[d]:
                    block = at(r - d * step, p)
                    copies.start((d, step + 1, p), block, block, to[d])
    for d in (RIGHT, LEFT):
        for p in last[d]:
            copies.arrived((d, 4, p))
    for copy in mine:
        copy.wait()
    copies.all_sent()


def gather_group(x, out_shape, place, n_pieces, collective_id):
    n = 7 * n_pieces
    return pl.pallas_call(
        functools.partial(group_kernel, place, n_pieces),
        out_shape=jax.ShapeDtypeStruct(out_shape, x.dtype),
        in_specs=[pl.BlockSpec(memory_space=pltpu.VMEM)],
        out_specs=pl.BlockSpec(memory_space=pl.ANY),
        scratch_shapes=[pltpu.SemaphoreType.DMA((n,)), pltpu.SemaphoreType.DMA((n,)), pltpu.SemaphoreType.DMA((n_pieces,))],
        compiler_params=pltpu.CompilerParams(collective_id=collective_id, has_side_effects=True),
    )(x)


def world_kernel(place, x_ref, out_ref, send_sem, recv_sem, own_sem):
    f, m = lax.axis_index('fsdp'), lax.axis_index('model')
    r = ring_place(f)
    other_m, core_m = (m + 2) % 4, m + 1 - 2 * (m % 2)
    to = {d: (ring_member((r + d + 8) % 8), m) for d in (RIGHT, LEFT)}
    to_plane, to_core = (f, other_m), (f, core_m)
    copies = Copies(send_sem, recv_sem)
    rows = x_ref.shape[0]
    half, quarter = rows // 2, rows // 4
    span = {'a': (0, half), 'b': (half, half), 'x': (0, half)}

    def at(member, origin, lo, n):
        return place(out_ref, member, ring_member((origin + 8) % 8), lo, n)

    def forward(name, block, device):
        copies.start(name, block, block, device)

    greet([to[RIGHT], to[LEFT], to_plane, to_core])
    copies.start('x0', x_ref.at[pl.ds(0, half)], at(m, r, 0, half), to_plane)
    for piece in 'ab':
        for d in (RIGHT, LEFT):
            copies.start((d, 1, piece), x_ref.at[pl.ds(*span[piece])], at(m, r, *span[piece]), to[d])
    copies.start(('x1', 0), x_ref.at[pl.ds(half, half)], at(m, r, half, half), to_plane)
    copies.start('core_own', x_ref, at(m, r, 0, rows), to_core)
    mine = pltpu.make_async_copy(x_ref, at(m, r, 0, rows), own_sem)
    mine.start()
    to_core_names = ['core_own']

    def share(name, block):
        name = ('core', name)
        forward(name, block, to_core)
        to_core_names.append(name)

    copies.arrived('x0')
    first = at(other_m, r, 0, half)
    for d in (RIGHT, LEFT):
        forward((d, 1, 'x'), first, to[d])
    share('x0', first)
    crossing = [0]
    for step in (1, 2, 3):
        for piece in 'abx':
            for d in (RIGHT, LEFT):
                copies.arrived((d, step, piece))
                origin, member = r - d * step, other_m if piece == 'x' else m
                block = at(member, origin, *span[piece])
                if step < 3:
                    forward((d, step + 1, piece), block, to[d])
                elif piece == 'x':
                    forward((d, 4, 'x'), at(member, origin, 0 if d == RIGHT else quarter, quarter), to[d])
                elif (piece == 'a') == (d == RIGHT):
                    forward((d, 4, piece), block, to[d])
                if piece == 'b':
                    forward(('x1', d * step), block, to_plane)
                    crossing.append(d * step)
                share((d, step, piece), block)
    copies.arrived((LEFT, 4, 'b'))
    block = at(m, r + 4, half, half)
    forward(('x1', 4), block, to_plane)
    crossing.append(4)
    share('b4', block)
    copies.arrived((RIGHT, 4, 'a'))
    share('a4', at(m, r + 4, 0, half))
    copies.arrived((RIGHT, 4, 'x'))
    copies.arrived((LEFT, 4, 'x'))
    share('x4', at(other_m, r + 4, 0, half))
    for away in crossing:
        copies.arrived(('x1', away))
        share(('x1', away), at(other_m, r - away, half, half))
    for name in to_core_names:
        copies.arrived(name)
    mine.wait()
    copies.all_sent()


def gather_world(x, out_shape, place, collective_id):
    n = 96
    return pl.pallas_call(
        functools.partial(world_kernel, place),
        out_shape=jax.ShapeDtypeStruct(out_shape, x.dtype),
        in_specs=[pl.BlockSpec(memory_space=pltpu.VMEM)],
        out_specs=pl.BlockSpec(memory_space=pl.ANY),
        scratch_shapes=[pltpu.SemaphoreType.DMA((n,)), pltpu.SemaphoreType.DMA((n,)), pltpu.SemaphoreType.DMA],
        compiler_params=pltpu.CompilerParams(collective_id=collective_id, has_side_effects=True),
    )(x)


def solution(mesh):
    n_f, n_m = mesh.shape['fsdp'], mesh.shape['model']
    act_spec = P('fsdp', 'model', None)
    col_spec = P(None, 'fsdp', 'model')
    row_spec = P(None, 'model', 'fsdp')

    def device_step(x_in, gain_attn, gain_mlp, rope_cos, rope_sin, w_q, w_k, w_v, w_o, w_gate, w_up, w_down):
        n_b, n_s, d = x_in.shape
        seq = n_s * n_m
        hd = 2 * rope_cos.shape[1]
        kv = w_k.shape[-1] // hd
        grp = w_q.shape[-1] // (hd * kv)
        rows = n_b * n_s
        d_f = d // n_f
        tok_m, tok = n_f * rows, n_m * n_f * rows
        f, m = lax.axis_index('fsdp'), lax.axis_index('model')

        def shuffle_cols(w):
            return lax.all_to_all(w, 'fsdp', split_axis=1, concat_axis=0, tiled=True)

        def matmul(a, b):
            return jnp.dot(a, b, preferred_element_type=jnp.float32)

        def matmul_t(a_t, b):
            return lax.dot_general(a_t, b, (((0,), (0,)), ((), ())), preferred_element_type=jnp.float32)

        def place_rows(ref, member, group, lo, n):
            return ref.at[pl.ds(pl.multiple_of((member * n_f + group) * rows + lo, 16), n)]

        def place_block(ref, member, group, lo, n):
            return ref.at[pl.ds(pl.multiple_of(group * d_f + lo, 16), n), pl.ds(pl.multiple_of(member * tok_m, 128), tok_m)]

        def place_z(ref, group, p):
            n = d_f // 4
            return ref.at[pl.ds(p * n, n)] if group is None else ref.at[pl.ds(pl.multiple_of(group * d_f + p * n, 16), n)]

        def place_o(ref, group, p):
            return ref.at[p] if group is None else ref.at[p, group]

        def return_rows(part, residual):
            total = lax.psum_scatter(part, 'model', scatter_dimension=0, tiled=True)
            return (residual.astype(jnp.float32) + total).astype(jnp.bfloat16)

        n_layers = w_q.shape[0]
        w_qkv = [shuffle_cols(jnp.concatenate([w_q[l], w_k[l], w_v[l]], axis=1)) for l in range(n_layers)]
        w_gu = [
            shuffle_cols(jnp.concatenate([w_gate[l].reshape(d_f, n_f, -1), w_up[l].reshape(d_f, n_f, -1)], axis=2)).reshape(d, -1)
            for l in range(n_layers)
        ]
        for l in range(n_layers):
            if l == 0:
                x_all = gather_world(x_in.reshape(rows, d), (tok, d), place_rows, 2)
                own_m = lax.dynamic_slice_in_dim(x_all, m * tok_m, tok_m, 0)
                residual = lax.dynamic_slice_in_dim(own_m.T, f * d_f, d_f, 0).T
                qkv = matmul(rms_norm(x_all, gain_attn[l]), w_qkv[l])
            else:
                x_all = gather_world(residual.T, (d, tok), place_block, 3)
                qkv = matmul_t(rms_norm(x_all, gain_attn[l][:, None], 0), w_qkv[l])
            qkv = qkv.astype(jnp.bfloat16).reshape(n_m, n_f, rows, hd)
            qkv = lax.all_to_all(qkv, 'fsdp', split_axis=1, concat_axis=3, tiled=True)
            qkv = qkv.reshape(n_m, n_b, n_s, -1).transpose(1, 0, 2, 3).reshape(n_b, seq, -1)
            q = qkv[..., :kv * grp * hd].reshape(n_b, seq, kv, grp, hd)
            k = qkv[..., kv * grp * hd:kv * (grp + 1) * hd].reshape(n_b, seq, kv, hd)
            v = qkv[..., kv * (grp + 1) * hd:].reshape(n_b, seq, kv, hd)
            q = rotate(q, rope_cos[None, :, None, None, :], rope_sin[None, :, None, None, :])
            k = rotate(k, rope_cos[None, :, None, :], rope_sin[None, :, None, :])
            scores = jnp.einsum('bqkgd,bskd->bkgqs', q, k, preferred_element_type=jnp.float32) * hd ** -0.5
            pos = jnp.arange(seq)
            scores = jnp.where(pos[:, None] >= pos[None, :], scores, -jnp.inf)
            probs = jax.nn.softmax(scores, axis=-1).astype(jnp.bfloat16)
            o = jnp.einsum('bkgqs,bskd->bqkgd', probs, v, preferred_element_type=jnp.float32).astype(jnp.bfloat16)
            o = o.reshape(n_b, n_m, n_s, -1).transpose(1, 0, 2, 3).reshape(n_m, rows, -1)
            o = gather_group(o, (n_m, n_f, rows, o.shape[-1]), place_o, n_m, 1).reshape(tok, -1)
            residual = return_rows(matmul(o, w_o[l]), residual)
            m_all = gather_world(residual.T, (d, tok), place_block, 3)
            gu = matmul_t(rms_norm(m_all, gain_mlp[l][:, None], 0), w_gu[l])
            z = (jax.nn.silu(gu[:, :gu.shape[1] // 2]) * gu[:, gu.shape[1] // 2:]).astype(jnp.bfloat16)
            z_all = gather_group(z.T, (n_f * z.shape[1], tok), place_z, 4, 0)
            residual = return_rows(matmul_t(z_all, w_down[l]), residual)
        y = lax.all_to_all(residual, 'fsdp', split_axis=0, concat_axis=1, tiled=True)
        return y.reshape(n_b, n_s, d)

    return jax.shard_map(device_step, mesh=mesh, in_specs=(act_spec, P(), P(), P(), P(), col_spec, col_spec, col_spec, row_spec, col_spec, col_spec, row_spec), out_specs=act_spec, check_vma=False)
```

```python
import functools

import jax
import jax.numpy as jnp
from jax import lax
from jax.experimental import pallas as pl
from jax.experimental.pallas import tpu as pltpu
from jax.sharding import PartitionSpec as P

EPS = 1e-5
MESH = pl.DeviceIdType.MESH
RIGHT, LEFT = 1, -1


def rms_norm(rows, gain, axis=-1):
    rows_f = rows.astype(jnp.float32)
    mean_sq = jnp.mean(rows_f * rows_f, axis=axis, keepdims=True)
    return (rows_f * lax.rsqrt(mean_sq + EPS) * gain).astype(jnp.bfloat16)


def rotate(heads, cos, sin):
    half = heads.shape[-1] // 2
    heads_f = heads.astype(jnp.float32)
    a, b = heads_f[..., :half], heads_f[..., half:]
    return jnp.concatenate([a * cos - b * sin, b * cos + a * sin], axis=-1).astype(jnp.bfloat16)


def ring_place(f):
    y, z = f % 2, f // 2
    return z * (1 - y) + (7 - z) * y


def ring_member(r):
    h = r // 4
    return 2 * (r * (1 - h) + (7 - r) * h) + h


class Copies:
    def __init__(self, send_sem, recv_sem):
        self.send_sem, self.recv_sem, self.made = send_sem, recv_sem, {}

    def start(self, name, src, dst, device):
        k = len(self.made)
        copy = pltpu.make_async_remote_copy(src_ref=src, dst_ref=dst, send_sem=self.send_sem.at[k], recv_sem=self.recv_sem.at[k], device_id=device, device_id_type=MESH)
        copy.start()
        self.made[name] = copy

    def arrived(self, name):
        self.made[name].wait_recv()

    def all_sent(self):
        for copy in self.made.values():
            copy.wait_send()


def greet(devices):
    barrier = pltpu.get_barrier_semaphore()
    for device in devices:
        pl.semaphore_signal(barrier, inc=1, device_id=device, device_id_type=MESH)
    pl.semaphore_wait(barrier, len(devices))


def group_kernel(place, n_pieces, x_ref, out_ref, send_sem, recv_sem, own_sem):
    f, m = lax.axis_index('fsdp'), lax.axis_index('model')
    r = ring_place(f)
    to = {d: (ring_member((r + d + 8) % 8), m) for d in (RIGHT, LEFT)}
    copies = Copies(send_sem, recv_sem)

    def at(origin, p):
        return place(out_ref, ring_member((origin + 8) % 8), p)

    def own(p):
        return place(x_ref, None, p)

    greet([to[RIGHT], to[LEFT]])
    for p in range(n_pieces):
        for d in (RIGHT, LEFT):
            copies.start((d, 1, p), own(p), at(r, p), to[d])
    mine = [pltpu.make_async_copy(own(p), at(r, p), own_sem.at[p]) for p in range(n_pieces)]
    for copy in mine:
        copy.start()
    last = {RIGHT: range(n_pieces // 2), LEFT: range(n_pieces // 2, n_pieces)}
    for step in (1, 2, 3):
        for p in range(n_pieces):
            for d in (RIGHT, LEFT):
                copies.arrived((d, step, p))
                if step < 3 or p in last[d]:
                    block = at(r - d * step, p)
                    copies.start((d, step + 1, p), block, block, to[d])
    for d in (RIGHT, LEFT):
        for p in last[d]:
            copies.arrived((d, 4, p))
    for copy in mine:
        copy.wait()
    copies.all_sent()


def gather_group(x, out_shape, place, n_pieces, collective_id):
    n = 7 * n_pieces
    return pl.pallas_call(
        functools.partial(group_kernel, place, n_pieces),
        out_shape=jax.ShapeDtypeStruct(out_shape, x.dtype),
        in_specs=[pl.BlockSpec(memory_space=pltpu.VMEM)],
        out_specs=pl.BlockSpec(memory_space=pl.ANY),
        scratch_shapes=[pltpu.SemaphoreType.DMA((n,)), pltpu.SemaphoreType.DMA((n,)), pltpu.SemaphoreType.DMA((n_pieces,))],
        compiler_params=pltpu.CompilerParams(collective_id=collective_id, has_side_effects=True),
    )(x)


def neighbours():
    f, m = lax.axis_index('fsdp'), lax.axis_index('model')
    r = ring_place(f)
    to = {d: (ring_member((r + d + 8) % 8), m) for d in (RIGHT, LEFT)}
    return f, m, r, to, (f, (m + 2) % 4), (f, m + 1 - 2 * (m % 2))


def gather_rows(place, ready, x_ref, out_ref, copies, own_sem):
    _, m, r, to, to_plane, to_core = neighbours()
    other_m = (m + 2) % 4
    rows = x_ref.shape[0]
    half, quarter = rows // 2, rows // 4
    span = {'a': (0, half), 'b': (half, half), 'x': (0, half)}

    def at(member, origin, lo, n):
        return place(out_ref, member, ring_member((origin + 8) % 8), lo, n)

    def forward(name, block, device):
        copies.start(name, block, block, device)

    ready(0)
    copies.start('x0', x_ref.at[pl.ds(0, half)], at(m, r, 0, half), to_plane)
    for piece in 'ab':
        if piece == 'b':
            ready(1)
        for d in (RIGHT, LEFT):
            copies.start((d, 1, piece), x_ref.at[pl.ds(*span[piece])], at(m, r, *span[piece]), to[d])
    copies.start(('x1', 0), x_ref.at[pl.ds(half, half)], at(m, r, half, half), to_plane)
    copies.start('core_own', x_ref, at(m, r, 0, rows), to_core)
    mine = pltpu.make_async_copy(x_ref, at(m, r, 0, rows), own_sem)
    mine.start()
    to_core_names = ['core_own']

    def share(name, block):
        name = ('core', name)
        forward(name, block, to_core)
        to_core_names.append(name)

    copies.arrived('x0')
    first = at(other_m, r, 0, half)
    for d in (RIGHT, LEFT):
        forward((d, 1, 'x'), first, to[d])
    share('x0', first)
    crossing = [0]
    for step in (1, 2, 3):
        for piece in 'abx':
            for d in (RIGHT, LEFT):
                copies.arrived((d, step, piece))
                origin, member = r - d * step, other_m if piece == 'x' else m
                block = at(member, origin, *span[piece])
                if step < 3:
                    forward((d, step + 1, piece), block, to[d])
                elif piece == 'x':
                    forward((d, 4, 'x'), at(member, origin, 0 if d == RIGHT else quarter, quarter), to[d])
                elif (piece == 'a') == (d == RIGHT):
                    forward((d, 4, piece), block, to[d])
                if piece == 'b':
                    forward(('x1', d * step), block, to_plane)
                    crossing.append(d * step)
                share((d, step, piece), block)
    copies.arrived((LEFT, 4, 'b'))
    block = at(m, r + 4, half, half)
    forward(('x1', 4), block, to_plane)
    crossing.append(4)
    share('b4', block)
    copies.arrived((RIGHT, 4, 'a'))
    share('a4', at(m, r + 4, 0, half))
    copies.arrived((RIGHT, 4, 'x'))
    copies.arrived((LEFT, 4, 'x'))
    share('x4', at(other_m, r + 4, 0, half))
    for away in crossing:
        copies.arrived(('x1', away))
        share(('x1', away), at(other_m, r - away, half, half))
    for name in to_core_names:
        copies.arrived(name)
    mine.wait()


def greet_world():
    _, _, _, to, to_plane, to_core = neighbours()
    greet([to[RIGHT], to[LEFT], to_plane, to_core])


def world_kernel(place, x_ref, out_ref, send_sem, recv_sem, own_sem):
    copies = Copies(send_sem, recv_sem)
    greet_world()
    gather_rows(place, lambda h: None, x_ref, out_ref, copies, own_sem)
    copies.all_sent()


def gather_world(x, out_shape, place, collective_id):
    n = 80
    return pl.pallas_call(
        functools.partial(world_kernel, place),
        out_shape=jax.ShapeDtypeStruct(out_shape, x.dtype),
        in_specs=[pl.BlockSpec(memory_space=pltpu.VMEM)],
        out_specs=pl.BlockSpec(memory_space=pl.ANY),
        scratch_shapes=[pltpu.SemaphoreType.DMA((n,)), pltpu.SemaphoreType.DMA((n,)), pltpu.SemaphoreType.DMA],
        compiler_params=pltpu.CompilerParams(collective_id=collective_id, has_side_effects=True),
    )(x)


PIECES = 4


def sum_kernel(place, part_ref, old_ref, *refs):
    if place:
        all_ref, new_ref, core_ref, sent_ref, came_ref, send_sem, recv_sem, own_sem = refs
    else:
        new_ref, core_ref, sent_ref, came_ref, send_sem, recv_sem = refs
    _, m, _, _, to_plane, to_core = neighbours()
    copies = Copies(send_sem, recv_sem)
    n, width = new_ref.shape[0] // PIECES, new_ref.shape[1]
    other_m = (m + 2) % 4
    core_m = m + 1 - 2 * (m % 2)

    def rows(p):
        return pl.ds(p * n, n)

    def columns(member):
        return pl.ds(pl.multiple_of(member * width, 128), width)

    if place:
        greet_world()
    else:
        greet([to_plane, to_core])
    for k, member in enumerate(((core_m + 2) % 4, core_m)):
        for p in range(PIECES):
            copies.start(('core', k, p), part_ref.at[rows(p), columns(member)], core_ref.at[k, rows(p)], to_core)

    def cross(p):
        copies.start(('cross', p), sent_ref.at[rows(p)], came_ref.at[rows(p)], to_plane)

    for p in range(PIECES):
        copies.arrived(('core', 0, p))
        sent_ref[rows(p), :] = part_ref[rows(p), columns(other_m)] + core_ref[0, rows(p), :]
        if p:
            cross(p - 1)
    for p in range(PIECES):
        copies.arrived(('core', 1, p))
        core_ref[1, rows(p), :] = part_ref[rows(p), columns(m)] + core_ref[1, rows(p), :]
        if p == 0:
            cross(PIECES - 1)

    def ready(h):
        for p in range(h * PIECES // 2, (h + 1) * PIECES // 2):
            copies.arrived(('cross', p))
            total = core_ref[1, rows(p), :] + came_ref[rows(p), :]
            new_ref[rows(p), :] = (old_ref[rows(p), :].astype(jnp.float32) + total).astype(new_ref.dtype)

    if place:
        gather_rows(place, ready, new_ref, all_ref, copies, own_sem)
    else:
        ready(0)
        ready(1)
    copies.all_sent()


def sum_rows(part, old, collective_id, place=None, all_shape=None):
    n = 3 * PIECES + (80 if place else 0)
    rows, width = old.shape
    vmem = pl.BlockSpec(memory_space=pltpu.VMEM)
    new = jax.ShapeDtypeStruct(old.shape, old.dtype)
    scratch = [
        pltpu.VMEM((2, rows, width), jnp.float32),
        pltpu.VMEM((rows, width), jnp.float32),
        pltpu.VMEM((rows, width), jnp.float32),
        pltpu.SemaphoreType.DMA((n,)),
        pltpu.SemaphoreType.DMA((n,)),
    ]
    return pl.pallas_call(
        functools.partial(sum_kernel, place),
        out_shape=[jax.ShapeDtypeStruct(all_shape, old.dtype), new] if place else new,
        in_specs=[vmem, vmem],
        out_specs=[pl.BlockSpec(memory_space=pl.ANY), vmem] if place else vmem,
        scratch_shapes=scratch + ([pltpu.SemaphoreType.DMA] if place else []),
        compiler_params=pltpu.CompilerParams(collective_id=collective_id, has_side_effects=True),
    )(part, old)


def solution(mesh):
    n_f, n_m = mesh.shape['fsdp'], mesh.shape['model']
    act_spec = P('fsdp', 'model', None)
    col_spec = P(None, 'fsdp', 'model')
    row_spec = P(None, 'model', 'fsdp')

    def device_step(x_in, gain_attn, gain_mlp, rope_cos, rope_sin, w_q, w_k, w_v, w_o, w_gate, w_up, w_down):
        n_b, n_s, d = x_in.shape
        seq = n_s * n_m
        hd = 2 * rope_cos.shape[1]
        kv = w_k.shape[-1] // hd
        grp = w_q.shape[-1] // (hd * kv)
        rows = n_b * n_s
        d_f = d // n_f
        tok_m, tok = n_f * rows, n_m * n_f * rows
        f, m = lax.axis_index('fsdp'), lax.axis_index('model')

        def matmul(a, b):
            return jnp.dot(a, b, preferred_element_type=jnp.float32)

        def matmul_t(a_t, b):
            return lax.dot_general(a_t, b, (((0,), (0,)), ((), ())), preferred_element_type=jnp.float32)

        def place_rows(ref, member, group, lo, n):
            return ref.at[pl.ds(pl.multiple_of((member * n_f + group) * rows + lo, 16), n)]

        def place_block(ref, member, group, lo, n):
            return ref.at[pl.ds(pl.multiple_of(group * d_f + lo, 16), n), pl.ds(pl.multiple_of(member * tok_m, 128), tok_m)]

        def place_z(ref, group, p):
            n = d_f // 4
            return ref.at[pl.ds(p * n, n)] if group is None else ref.at[pl.ds(pl.multiple_of(group * d_f + p * n, 16), n)]

        def place_o(ref, group, p):
            return ref.at[p] if group is None else ref.at[p, group]

        n_layers = w_q.shape[0]
        ff = w_gate.shape[-1] // n_f
        cut = 256

        def block(l, name):
            if name == 'qkv':
                whole = jnp.concatenate([w_q[l], w_k[l], w_v[l]], axis=1)
                return whole.reshape(d_f, n_f, -1).transpose(1, 0, 2)
            part = slice(0, cut) if name == 'a' else slice(cut, ff)
            both = [w[l].reshape(d_f, n_f, ff)[:, :, part] for w in (w_gate, w_up)]
            return jnp.concatenate(both, axis=2).transpose(1, 0, 2)

        dealt, newest = {}, []

        def settled(*values):
            values = lax.optimization_barrier(values + tuple(dealt[k] for k in newest))
            for k in newest:
                dealt[k] = values[-1]
            newest.clear()
            return values

        def deal(l, name, after):
            after, w = settled(after, block(l, name))[:2]
            dealt[l, name] = lax.all_to_all(w, 'fsdp', split_axis=0, concat_axis=0, tiled=True).reshape(d, -1)
            newest.append((l, name))
            return after

        def layer(l, x_all, residual):
            last = l == n_layers - 1
            if l == 0:
                qkv = matmul(rms_norm(x_all, gain_attn[l]), dealt[l, 'qkv'])
            else:
                qkv = matmul_t(rms_norm(x_all, gain_attn[l][:, None], 0), dealt[l, 'qkv'])
            qkv = qkv.astype(jnp.bfloat16).reshape(n_m, n_f, rows, hd)
            qkv = lax.all_to_all(settled(qkv)[0], 'fsdp', split_axis=1, concat_axis=3, tiled=True)
            if l == 0:
                qkv = deal(l, 'a', qkv)
            qkv = qkv.reshape(n_m, n_b, n_s, -1).transpose(1, 0, 2, 3).reshape(n_b, seq, -1)
            q = qkv[..., :kv * grp * hd].reshape(n_b, seq, kv, grp, hd)
            k = qkv[..., kv * grp * hd:kv * (grp + 1) * hd].reshape(n_b, seq, kv, hd)
            v = qkv[..., kv * (grp + 1) * hd:].reshape(n_b, seq, kv, hd)
            q = rotate(q, rope_cos[None, :, None, None, :], rope_sin[None, :, None, None, :])
            k = rotate(k, rope_cos[None, :, None, :], rope_sin[None, :, None, :])
            scores = jnp.einsum('bqkgd,bskd->bkgqs', q, k, preferred_element_type=jnp.float32) * hd ** -0.5
            pos = jnp.arange(seq)
            scores = jnp.where(pos[:, None] >= pos[None, :], scores, -jnp.inf)
            probs = jax.nn.softmax(scores, axis=-1).astype(jnp.bfloat16)
            o = jnp.einsum('bkgqs,bskd->bqkgd', probs, v, preferred_element_type=jnp.float32).astype(jnp.bfloat16)
            o = o.reshape(n_b, n_m, n_s, -1).transpose(1, 0, 2, 3).reshape(n_m, rows, -1)
            o = gather_group(o, (n_m, n_f, rows, o.shape[-1]), place_o, n_m, 1).reshape(tok, -1)
            o = deal(l, 'b', o)
            part = matmul(o, w_o[l]).T
            m_all, residual = sum_rows(part, residual, 3, place_block, (d, tok))
            if not last:
                m_all = deal(l + 1, 'qkv', m_all)
            u = rms_norm(m_all, gain_mlp[l][:, None], 0)
            z = []
            for name in 'ab':
                gu = matmul_t(u, dealt[l, name])
                n = gu.shape[1] // 2
                z.append((jax.nn.silu(gu[:, :n]) * gu[:, n:]).astype(jnp.bfloat16).T)
            z_all = gather_group(jnp.concatenate(z, axis=0), (n_f * ff, tok), place_z, 4, 0)
            if not last:
                z_all = deal(l + 1, 'a', z_all)
            part = matmul_t(z_all, w_down[l]).T
            if not last:
                return sum_rows(part, residual, 3, place_block, (d, tok))
            return None, sum_rows(part, residual, 4)

        x_rows = deal(0, 'qkv', x_in.reshape(rows, d))
        x_all = gather_world(x_rows, (tok, d), place_rows, 2)
        own_m = lax.dynamic_slice_in_dim(x_all, m * tok_m, tok_m, 0)
        residual = lax.dynamic_slice_in_dim(own_m.T, f * d_f, d_f, 0)
        for l in range(n_layers):
            x_all, residual = layer(l, x_all, residual)
        y = lax.all_to_all(residual.T, 'fsdp', split_axis=0, concat_axis=1, tiled=True)
        return y.reshape(n_b, n_s, d)

    return jax.shard_map(device_step, mesh=mesh, in_specs=(act_spec, P(), P(), P(), P(), col_spec, col_spec, col_spec, row_spec, col_spec, col_spec, row_spec), out_specs=act_spec, check_vma=False)
```

```python
import functools

import jax
import jax.numpy as jnp
from jax import lax
from jax.experimental import pallas as pl
from jax.experimental.pallas import tpu as pltpu
from jax.sharding import PartitionSpec as P

EPS = 1e-5
MESH = pl.DeviceIdType.MESH
RIGHT, LEFT = 1, -1


def rms_norm(rows, gain):
    rows_f = rows.astype(jnp.float32)
    mean_sq = jnp.mean(rows_f * rows_f, axis=-1, keepdims=True)
    return (rows_f * lax.rsqrt(mean_sq + EPS) * gain).astype(jnp.bfloat16)


def rms_norm_t(columns, gain):
    columns_f = columns.astype(jnp.float32)
    mean_sq = jnp.mean(columns_f * columns_f, axis=0, keepdims=True)
    return (columns_f * lax.rsqrt(mean_sq + EPS) * gain[:, None]).astype(jnp.bfloat16)


def rotate(heads, cos, sin):
    half = heads.shape[-1] // 2
    heads_f = heads.astype(jnp.float32)
    a, b = heads_f[..., :half], heads_f[..., half:]
    return jnp.concatenate([a * cos - b * sin, b * cos + a * sin], axis=-1).astype(jnp.bfloat16)


def ring_place(f):
    y, z = f % 2, f // 2
    return z * (1 - y) + (7 - z) * y


def ring_member(r):
    h = r // 4
    return 2 * (r * (1 - h) + (7 - r) * h) + h


class Copies:
    def __init__(self, send_sem, recv_sem):
        self.send_sem, self.recv_sem, self.made = send_sem, recv_sem, {}

    def start(self, name, src, dst, device):
        k = len(self.made)
        copy = pltpu.make_async_remote_copy(src_ref=src, dst_ref=dst, send_sem=self.send_sem.at[k], recv_sem=self.recv_sem.at[k], device_id=device, device_id_type=MESH)
        copy.start()
        self.made[name] = copy

    def arrived(self, name):
        self.made[name].wait_recv()

    def all_sent(self):
        for copy in self.made.values():
            copy.wait_send()


def greet(devices):
    barrier = pltpu.get_barrier_semaphore()
    for device in devices:
        pl.semaphore_signal(barrier, inc=1, device_id=device, device_id_type=MESH)
    pl.semaphore_wait(barrier, len(devices))


def neighbours():
    f, m = lax.axis_index('fsdp'), lax.axis_index('model')
    r = ring_place(f)
    to = {d: (ring_member((r + d + 8) % 8), m) for d in (RIGHT, LEFT)}
    return f, m, r, to, (f, (m + 2) % 4), (f, m + 1 - 2 * (m % 2))


def gather_blocks(place, n_pieces, x_ref, out_ref, copies, own_sem):
    _, _, r, to, _, _ = neighbours()

    def at(origin, p):
        return place(out_ref, ring_member((origin + 8) % 8), p)

    def own(p):
        return place(x_ref, None, p)

    for p in range(n_pieces):
        for d in (RIGHT, LEFT):
            copies.start((d, 1, p), own(p), at(r, p), to[d])
    mine = [pltpu.make_async_copy(own(p), at(r, p), own_sem.at[p]) for p in range(n_pieces)]
    for copy in mine:
        copy.start()
    last = {RIGHT: range(n_pieces // 2), LEFT: range(n_pieces // 2, n_pieces)}
    for step in (1, 2, 3):
        for p in range(n_pieces):
            for d in (RIGHT, LEFT):
                copies.arrived((d, step, p))
                if step < 3 or p in last[d]:
                    block = at(r - d * step, p)
                    copies.start((d, step + 1, p), block, block, to[d])
    for d in (RIGHT, LEFT):
        for p in last[d]:
            copies.arrived((d, 4, p))
    for copy in mine:
        copy.wait()


def group_kernel(place, n_pieces, x_ref, out_ref, send_sem, recv_sem, own_sem):
    _, _, _, to, _, _ = neighbours()
    copies = Copies(send_sem, recv_sem)
    greet([to[RIGHT], to[LEFT]])
    gather_blocks(place, n_pieces, x_ref, out_ref, copies, own_sem)
    copies.all_sent()


def gather_group(x, out_shape, place, n_pieces, collective_id):
    n = 7 * n_pieces
    return pl.pallas_call(
        functools.partial(group_kernel, place, n_pieces),
        out_shape=jax.ShapeDtypeStruct(out_shape, x.dtype),
        in_specs=[pl.BlockSpec(memory_space=pltpu.VMEM)],
        out_specs=pl.BlockSpec(memory_space=pl.ANY),
        scratch_shapes=[pltpu.SemaphoreType.DMA((n,)), pltpu.SemaphoreType.DMA((n,)), pltpu.SemaphoreType.DMA((n_pieces,))],
        compiler_params=pltpu.CompilerParams(collective_id=collective_id, has_side_effects=True),
    )(x)


def attend_kernel(place, kv, qkv_ref, cos_ref, sin_ref, out_ref, got_ref, o_ref, send_sem, recv_sem, own_sem):
    f, m, _, _, _, _ = neighbours()
    n_f, n_m, n_rows, hd = got_ref.shape
    grp = o_ref.shape[-1] // (hd * kv)
    n_s = cos_ref.shape[0] // n_m
    copies = Copies(send_sem, recv_sem)
    members = [(f + j) % n_f for j in range(1, n_f)]
    greet([(g, m) for g in members])
    for j, g in enumerate(members):
        copies.start(('head', j), qkv_ref.at[:, g], got_ref.at[f], (g, m))
    for i in range(n_m):
        got_ref[f, i] = qkv_ref[i, f]
    for j in range(n_f - 1):
        copies.arrived(('head', j))
    cos, sin = cos_ref[...], sin_ref[...]
    seq = n_m * n_s
    at_query = lax.broadcasted_iota(jnp.int32, (grp * seq, seq), 0) % seq
    seen = at_query >= lax.broadcasted_iota(jnp.int32, (grp * seq, seq), 1)

    for b in range(n_rows // n_s):
        rows = pl.ds(b * n_s, n_s)

        def head(c):
            return jnp.concatenate([got_ref[c, i, rows, :] for i in range(n_m)], axis=0)

        for h in range(kv):
            k = rotate(head(kv * grp + h), cos, sin)
            v = head(kv * (grp + 1) + h)
            q = jnp.concatenate([rotate(head(h * grp + g), cos, sin) for g in range(grp)], axis=0)
            scores = lax.dot_general(q, k, (((1,), (1,)), ((), ())), preferred_element_type=jnp.float32) * hd ** -0.5
            scores = jnp.where(seen, scores, -jnp.inf)
            grown = jnp.exp(scores - jnp.max(scores, axis=-1, keepdims=True))
            probs = (grown / jnp.sum(grown, axis=-1, keepdims=True)).astype(jnp.bfloat16)
            o = jnp.dot(probs, v, preferred_element_type=jnp.float32).astype(jnp.bfloat16)
            for g in range(grp):
                for i in range(n_m):
                    o_ref[i, rows, pl.ds((h * grp + g) * hd, hd)] = o[g * seq + i * n_s:g * seq + (i + 1) * n_s]
    gather_blocks(place, n_m, o_ref, out_ref, copies, own_sem)
    copies.all_sent()


def attend(qkv, cos, sin, kv, width, place, collective_id):
    n_m, n_f, n_rows, hd = qkv.shape
    n = 7 * n_m + n_f - 1
    vmem = pl.BlockSpec(memory_space=pltpu.VMEM)
    return pl.pallas_call(
        functools.partial(attend_kernel, place, kv),
        out_shape=jax.ShapeDtypeStruct((n_m, n_f, n_rows, width), qkv.dtype),
        in_specs=[vmem, vmem, vmem],
        out_specs=pl.BlockSpec(memory_space=pl.ANY),
        scratch_shapes=[
            pltpu.VMEM((n_f, n_m, n_rows, hd), qkv.dtype),
            pltpu.VMEM((n_m, n_rows, width), qkv.dtype),
            pltpu.SemaphoreType.DMA((n,)),
            pltpu.SemaphoreType.DMA((n,)),
            pltpu.SemaphoreType.DMA((n_m,)),
        ],
        compiler_params=pltpu.CompilerParams(collective_id=collective_id, has_side_effects=True),
    )(qkv, cos, sin)


def sort_heads_kernel(q_ref, k_ref, v_ref, out_ref):
    hd = out_ref.shape[-1]
    c = 0
    for ref in (q_ref, k_ref, v_ref):
        for i in range(ref.shape[-1] // hd):
            out_ref[c] = ref[0, :, i * hd:(i + 1) * hd]
            c += 1


def sort_heads(l, n_f, w_q, w_k, w_v):
    d_f = w_q.shape[1]
    hd = (w_q.shape[2] + w_k.shape[2] + w_v.shape[2]) // n_f
    tile = d_f // 4
    spec = lambda w: pl.BlockSpec((1, tile, w.shape[2]), lambda i: (l, i, 0))
    return pl.pallas_call(
        sort_heads_kernel,
        grid=(d_f // tile,),
        out_shape=jax.ShapeDtypeStruct((n_f, d_f, hd), w_q.dtype),
        in_specs=[spec(w_q), spec(w_k), spec(w_v)],
        out_specs=pl.BlockSpec((n_f, tile, hd), lambda i: (0, i, 0)),
    )(w_q, w_k, w_v)


def sort_hidden_kernel(cut, gate_ref, up_ref, a_ref, b_ref):
    n_f = a_ref.shape[0]
    ff = gate_ref.shape[-1] // n_f
    for f in range(n_f):
        for k, ref in enumerate((gate_ref, up_ref)):
            w = ref[0, :, f * ff:(f + 1) * ff]
            a_ref[f, :, k * cut:(k + 1) * cut] = w[:, :cut]
            b_ref[f, :, k * (ff - cut):(k + 1) * (ff - cut)] = w[:, cut:]


def sort_hidden(l, n_f, cut, w_gate, w_up):
    d_f, width = w_gate.shape[1:]
    ff = width // n_f
    tile = d_f // 14
    spec = pl.BlockSpec((1, tile, width), lambda i: (l, i, 0))
    sizes = (2 * cut, 2 * (ff - cut))
    return pl.pallas_call(
        functools.partial(sort_hidden_kernel, cut),
        grid=(d_f // tile,),
        out_shape=[jax.ShapeDtypeStruct((n_f, d_f, n), w_gate.dtype) for n in sizes],
        in_specs=[spec, spec],
        out_specs=[pl.BlockSpec((n_f, tile, n), lambda i: (0, i, 0)) for n in sizes],
    )(w_gate, w_up)


def gather_rows(place, ready, x_ref, out_ref, copies, own_sem):
    _, m, r, to, to_plane, to_core = neighbours()
    other_m = (m + 2) % 4
    rows = x_ref.shape[0]
    half, quarter = rows // 2, rows // 4
    span = {'a': (0, half), 'b': (half, half), 'x': (0, half)}

    def at(member, origin, lo, n):
        return place(out_ref, member, ring_member((origin + 8) % 8), lo, n)

    def forward(name, block, device):
        copies.start(name, block, block, device)

    ready(0)
    copies.start('x0', x_ref.at[pl.ds(0, half)], at(m, r, 0, half), to_plane)
    for piece in 'ab':
        if piece == 'b':
            ready(1)
        for d in (RIGHT, LEFT):
            copies.start((d, 1, piece), x_ref.at[pl.ds(*span[piece])], at(m, r, *span[piece]), to[d])
    copies.start(('x1', 0), x_ref.at[pl.ds(half, half)], at(m, r, half, half), to_plane)
    copies.start('core_own', x_ref, at(m, r, 0, rows), to_core)
    mine = pltpu.make_async_copy(x_ref, at(m, r, 0, rows), own_sem)
    mine.start()
    to_core_names = ['core_own']

    def share(name, block):
        name = ('core', name)
        forward(name, block, to_core)
        to_core_names.append(name)

    copies.arrived('x0')
    first = at(other_m, r, 0, half)
    for d in (RIGHT, LEFT):
        forward((d, 1, 'x'), first, to[d])
    share('x0', first)
    crossing = [0]
    for step in (1, 2, 3):
        for piece in 'abx':
            for d in (RIGHT, LEFT):
                copies.arrived((d, step, piece))
                origin, member = r - d * step, other_m if piece == 'x' else m
                block = at(member, origin, *span[piece])
                if step < 3:
                    forward((d, step + 1, piece), block, to[d])
                elif piece == 'x':
                    forward((d, 4, 'x'), at(member, origin, 0 if d == RIGHT else quarter, quarter), to[d])
                elif (piece == 'a') == (d == RIGHT):
                    forward((d, 4, piece), block, to[d])
                if piece == 'b':
                    forward(('x1', d * step), block, to_plane)
                    crossing.append(d * step)
                share((d, step, piece), block)
    copies.arrived((LEFT, 4, 'b'))
    block = at(m, r + 4, half, half)
    forward(('x1', 4), block, to_plane)
    crossing.append(4)
    share('b4', block)
    copies.arrived((RIGHT, 4, 'a'))
    share('a4', at(m, r + 4, 0, half))
    copies.arrived((RIGHT, 4, 'x'))
    copies.arrived((LEFT, 4, 'x'))
    share('x4', at(other_m, r + 4, 0, half))
    for away in crossing:
        copies.arrived(('x1', away))
        share(('x1', away), at(other_m, r - away, half, half))
    for name in to_core_names:
        copies.arrived(name)
    mine.wait()


def greet_world():
    _, _, _, to, to_plane, to_core = neighbours()
    greet([to[RIGHT], to[LEFT], to_plane, to_core])


def world_kernel(place, x_ref, out_ref, send_sem, recv_sem, own_sem):
    copies = Copies(send_sem, recv_sem)
    greet_world()
    gather_rows(place, lambda h: None, x_ref, out_ref, copies, own_sem)
    copies.all_sent()


def gather_world(x, out_shape, place, collective_id):
    n = 80
    return pl.pallas_call(
        functools.partial(world_kernel, place),
        out_shape=jax.ShapeDtypeStruct(out_shape, x.dtype),
        in_specs=[pl.BlockSpec(memory_space=pltpu.VMEM)],
        out_specs=pl.BlockSpec(memory_space=pl.ANY),
        scratch_shapes=[pltpu.SemaphoreType.DMA((n,)), pltpu.SemaphoreType.DMA((n,)), pltpu.SemaphoreType.DMA],
        compiler_params=pltpu.CompilerParams(collective_id=collective_id, has_side_effects=True),
    )(x)


PIECES = 4


def sum_kernel(place, part_ref, old_ref, *refs):
    if place:
        all_ref, new_ref, core_ref, sent_ref, came_ref, send_sem, recv_sem, own_sem = refs
    else:
        new_ref, core_ref, sent_ref, came_ref, send_sem, recv_sem = refs
    _, m, _, _, to_plane, to_core = neighbours()
    copies = Copies(send_sem, recv_sem)
    n, width = new_ref.shape[0] // PIECES, new_ref.shape[1]
    other_m = (m + 2) % 4
    core_m = m + 1 - 2 * (m % 2)

    def rows(p):
        return pl.ds(p * n, n)

    def columns(member):
        return pl.ds(pl.multiple_of(member * width, 128), width)

    if place:
        greet_world()
    else:
        greet([to_plane, to_core])
    for k, member in enumerate(((core_m + 2) % 4, core_m)):
        for p in range(PIECES):
            copies.start(('core', k, p), part_ref.at[rows(p), columns(member)], core_ref.at[k, rows(p)], to_core)

    def cross(p):
        copies.start(('cross', p), sent_ref.at[rows(p)], came_ref.at[rows(p)], to_plane)

    for p in range(PIECES):
        copies.arrived(('core', 0, p))
        sent_ref[rows(p), :] = part_ref[rows(p), columns(other_m)] + core_ref[0, rows(p), :]
        if p:
            cross(p - 1)
    for p in range(PIECES):
        copies.arrived(('core', 1, p))
        core_ref[1, rows(p), :] = part_ref[rows(p), columns(m)] + core_ref[1, rows(p), :]
        if p == 0:
            cross(PIECES - 1)

    def ready(h):
        for p in range(h * PIECES // 2, (h + 1) * PIECES // 2):
            copies.arrived(('cross', p))
            total = core_ref[1, rows(p), :] + came_ref[rows(p), :]
            new_ref[rows(p), :] = (old_ref[rows(p), :].astype(jnp.float32) + total).astype(new_ref.dtype)

    if place:
        gather_rows(place, ready, new_ref, all_ref, copies, own_sem)
    else:
        ready(0)
        ready(1)
    copies.all_sent()


def sum_rows(part, old, collective_id, place=None, all_shape=None):
    n = 3 * PIECES + (80 if place else 0)
    rows, width = old.shape
    vmem = pl.BlockSpec(memory_space=pltpu.VMEM)
    new = jax.ShapeDtypeStruct(old.shape, old.dtype)
    scratch = [
        pltpu.VMEM((2, rows, width), jnp.float32),
        pltpu.VMEM((rows, width), jnp.float32),
        pltpu.VMEM((rows, width), jnp.float32),
        pltpu.SemaphoreType.DMA((n,)),
        pltpu.SemaphoreType.DMA((n,)),
    ]
    return pl.pallas_call(
        functools.partial(sum_kernel, place),
        out_shape=[jax.ShapeDtypeStruct(all_shape, old.dtype), new] if place else new,
        in_specs=[vmem, vmem],
        out_specs=[pl.BlockSpec(memory_space=pl.ANY), vmem] if place else vmem,
        scratch_shapes=scratch + ([pltpu.SemaphoreType.DMA] if place else []),
        compiler_params=pltpu.CompilerParams(collective_id=collective_id, has_side_effects=True),
    )(part, old)


def solution(mesh):
    n_f, n_m = mesh.shape['fsdp'], mesh.shape['model']
    act_spec = P('fsdp', 'model', None)
    col_spec = P(None, 'fsdp', 'model')
    row_spec = P(None, 'model', 'fsdp')

    def device_step(x_in, gain_attn, gain_mlp, rope_cos, rope_sin, w_q, w_k, w_v, w_o, w_gate, w_up, w_down):
        n_b, n_s, d = x_in.shape
        hd = 2 * rope_cos.shape[1]
        kv = w_k.shape[-1] // hd
        grp = w_q.shape[-1] // (hd * kv)
        rows = n_b * n_s
        d_f = d // n_f
        tok_m, tok = n_f * rows, n_m * n_f * rows
        f, m = lax.axis_index('fsdp'), lax.axis_index('model')

        def matmul(a, b):
            return jnp.dot(a, b, preferred_element_type=jnp.float32)

        def matmul_t(a_t, b):
            return lax.dot_general(a_t, b, (((0,), (0,)), ((), ())), preferred_element_type=jnp.float32)

        def place_rows(ref, member, group, lo, n):
            return ref.at[pl.ds(pl.multiple_of((member * n_f + group) * rows + lo, 16), n)]

        def place_block(ref, member, group, lo, n):
            return ref.at[pl.ds(pl.multiple_of(group * d_f + lo, 16), n), pl.ds(pl.multiple_of(member * tok_m, 128), tok_m)]

        def place_z(ref, group, p):
            n = d_f // 4
            return ref.at[pl.ds(p * n, n)] if group is None else ref.at[pl.ds(pl.multiple_of(group * d_f + p * n, 16), n)]

        def place_o(ref, group, p):
            return ref.at[p] if group is None else ref.at[p, group]

        n_layers = w_q.shape[0]
        ff = w_gate.shape[-1] // n_f
        cut = 256

        blocks = {}
        for l in range(n_layers):
            blocks[l, 'qkv'] = sort_heads(l, n_f, w_q, w_k, w_v)
            blocks[l, 'a'], blocks[l, 'b'] = sort_hidden(l, n_f, cut, w_gate, w_up)

        dealt, newest = {}, []

        def settled(*values):
            values = lax.optimization_barrier(values + tuple(dealt[k] for k in newest))
            for k in newest:
                dealt[k] = values[-1]
            newest.clear()
            return values

        def deal(l, name, after):
            after, w = settled(after, blocks[l, name])[:2]
            dealt[l, name] = lax.all_to_all(w, 'fsdp', split_axis=0, concat_axis=0, tiled=True).reshape(d, -1)
            newest.append((l, name))
            return after

        def layer(l, x_all, residual):
            last = l == n_layers - 1
            if l == 0:
                x_all = deal(l, 'a', x_all)
            if l == 0:
                qkv = matmul(rms_norm(x_all, gain_attn[l]), dealt[l, 'qkv'])
            else:
                qkv = matmul_t(rms_norm_t(x_all, gain_attn[l]), dealt[l, 'qkv'])
            qkv = qkv.astype(jnp.bfloat16).reshape(n_m, n_f, rows, hd)
            o = attend(qkv, rope_cos, rope_sin, kv, kv * grp * hd, place_o, 1).reshape(tok, -1)
            o = deal(l, 'b', o)
            part = matmul(o, w_o[l]).T
            m_all, residual = sum_rows(part, residual, 3, place_block, (d, tok))
            if not last:
                m_all = deal(l + 1, 'qkv', m_all)
            u = rms_norm_t(m_all, gain_mlp[l])
            z = []
            for name in 'ab':
                gu = matmul_t(u, dealt[l, name])
                n = gu.shape[1] // 2
                z.append((jax.nn.silu(gu[:, :n]) * gu[:, n:]).astype(jnp.bfloat16).T)
            z_all = gather_group(jnp.concatenate(z, axis=0), (n_f * ff, tok), place_z, 4, 0)
            if not last:
                z_all = deal(l + 1, 'a', z_all)
            part = matmul_t(z_all, w_down[l]).T
            if not last:
                return sum_rows(part, residual, 3, place_block, (d, tok))
            return None, sum_rows(part, residual, 4)

        x_rows = deal(0, 'qkv', x_in.reshape(rows, d))
        x_rows, blocks[0, 'a'], blocks[0, 'b'] = lax.optimization_barrier((x_rows, blocks[0, 'a'], blocks[0, 'b']))
        x_all = gather_world(x_rows, (tok, d), place_rows, 2)
        own_m = lax.dynamic_slice_in_dim(x_all, m * tok_m, tok_m, 0)
        residual = lax.dynamic_slice_in_dim(own_m.T, f * d_f, d_f, 0)
        for l in range(n_layers):
            x_all, residual = layer(l, x_all, residual)
        y = lax.all_to_all(residual.T, 'fsdp', split_axis=0, concat_axis=1, tiled=True)
        return y.reshape(n_b, n_s, d)

    return jax.shard_map(device_step, mesh=mesh, in_specs=(act_spec, P(), P(), P(), P(), col_spec, col_spec, col_spec, row_spec, col_spec, col_spec, row_spec), out_specs=act_spec, check_vma=False)
```
